256 devices in a mesh: ka: 8 (over z), row: 32 (over y, x, core).
Axes of the slice: x: 4, y: 4, z: 8, core: 2. Of those that a mesh axis runs over, the one named last changes fastest.
Arguments:
- hamiltonian: float32 [32768, 4096], P(('ka', 'row')), parts along dimension 0, as said below
Outputs:
- sign_next: float32 [32768, 4096], P(('ka', 'row')), parts along dimension 0
- occupation: float32 [8], P('ka'), parts along dimension 0
There are 8 independent parts, one for each index of `ka`. The reference program is written for one: setup_inputs(seed, part) draws one part's arguments, and reference() takes and returns one part's arrays. A program takes and returns all parts, laid end to end along the dimension named above; each array names one. Nothing has to cross between parts.
Inputs may be any that keep to these rules, and one draw needn't show every extreme that they name: hamiltonian is symmetric up to float32 rounding.
All inputs are finite; a program needn't handle non-finite values.
Results may differ from the reference program's by a relative error of at most 0.0038.
Values may be sent and summed in bfloat16 or wider, within the bound.
No kernel may reach another device: no remote copies, remote signals or barrier semaphores. Data moves between devices by JAX's collectives and lax.ppermute only.
A program may use at most 128 MiB of HBM per device.

```python
import math
import jax
import jax.numpy as jnp

N = 4096


def draw_hamiltonian(key, part):
    subkeys = jax.random.split(key, 4)
    channel_size = N // 2
    positions = jnp.arange(N, dtype=jnp.int32)
    ramped = positions.astype(jnp.float32) / N
    onsite = -0.3 + 1.2 * ramped + 0.15 * jax.random.normal(subkeys[0], (N,), jnp.float32)
    disorder = jax.random.normal(subkeys[1], (N, N), jnp.float32)
    hopping = 0.25 * (0.6 + 0.8 * jax.random.uniform(subkeys[2], (N - 1,), jnp.float32))
    inside = ((positions[:-1] + 1) % channel_size != 0).astype(jnp.float32)
    hopping = hopping * inside
    coupling = 0.25 * (0.6 + 0.8 * jax.random.uniform(subkeys[3], (channel_size,), jnp.float32))
    disorder = disorder * (0.3 / math.sqrt(2.0 * N))
    couplings = jnp.diag(hopping, 1) + jnp.diag(coupling, channel_size)
    return jnp.diag(onsite) + couplings + couplings.T + disorder + disorder.T


def setup_inputs(seed: int = 0, part: int = 0) -> dict:
    splits = jax.random.split(jax.random.key(seed), 2)
    part_splits = jax.random.split(jax.random.fold_in(splits[1], part), 2)
    hamiltonian = draw_hamiltonian(jax.random.fold_in(jax.random.fold_in(splits[1], part), 71), part)
    return dict(hamiltonian=hamiltonian)


def reference(hamiltonian):
    rounded = hamiltonian.astype(jnp.bfloat16)
    square = jnp.dot(rounded, rounded, preferred_element_type=jnp.float32).astype(jnp.bfloat16)
    cube = jnp.dot(square, rounded, preferred_element_type=jnp.float32)
    sign_next = 1.5 * hamiltonian - 0.5 * cube
    total = jnp.trace(sign_next)
    occupation = jnp.reshape(0.5 - total / (2.0 * N), (1,))
    return sign_next, occupation
```

```python
import jax
import jax.numpy as jnp
from jax import lax
from jax.experimental import pallas as pl
from jax.experimental.pallas import tpu as pltpu
from jax.sharding import Mesh
from jax.sharding import PartitionSpec as P

LOW = jnp.bfloat16
WIDE = jnp.float32
ANY = pl.BlockSpec(memory_space=pl.ANY)
VMEM = pl.BlockSpec(memory_space=pltpu.VMEM)
SIDE = 4
GRID = ("y", "x", "core")


def moved(y, x, core, axis, by):
    by = by if core == 0 else -by
    if (axis == "u") == (core == 0):
        return y, (x + by) % SIDE, core
    return (y + by) % SIDE, x, core


def index(y, x, core):
    return (y * SIDE + x) * 2 + core


PLACES = [(y, x, core) for y in range(SIDE) for x in range(SIDE) for core in range(2)]


def move(array, axis, by):
    return lax.ppermute(array, GRID, [(index(*p), index(*moved(*p, axis, by))) for p in PLACES])


def shift(array, axis, by):
    size = lax.axis_size(axis)
    return lax.ppermute(array, axis, [(i, (i + by) % size) for i in range(size)])


def swap(array):
    return shift(array, "core", 1)


def product(a, b, left=1, right=0):
    return lax.dot_general(a, b, (((left,), (right,)), ((), ())), preferred_element_type=WIDE)


def kernel(body, args, specs, outs, scratch, limit, flops):
    return pl.pallas_call(
        body,
        out_shape=[jax.ShapeDtypeStruct(*out) for out in outs],
        in_specs=specs,
        out_specs=[VMEM] * len(outs),
        scratch_shapes=scratch,
        compiler_params=pltpu.CompilerParams(vmem_limit_bytes=limit << 20),
        cost_estimate=pl.CostEstimate(flops=flops, bytes_accessed=1 << 20, transcendentals=0),
    )(*args)


def near_body(*refs):
    sources, (v, u, out, sems) = refs[:12], refs[12:]
    copies = []
    for n, source in enumerate(sources):
        target = (v if n < 6 else u).at[pl.ds(n % 6 * 128, 128), :]
        copies.append(pltpu.make_async_copy(source, target, sems.at[n]))
        copies[-1].start()
    for copy in copies:
        copy.wait()
    out[...] = product(v[...], u[...], 1, 1).astype(LOW)


def columns_of(core):
    return pl.ds(pl.multiple_of(core * 2048, 128), 2048)


def far_body(v, u, near, vc, vo, uc, uo, exact, side, up, down, trace, vf, uf, st, diagonal, sems):
    y, x, core = (lax.axis_index(a) for a in GRID)
    own = pl.multiple_of(((y * SIDE + x) * 2 + core) * 128, 128)
    copies = [pltpu.make_async_copy(exact.at[:, pl.ds(own, 128)], diagonal, sems.at[0])]
    for n, (source, target) in enumerate(((vc, vf), (vo, vf), (uc, uf), (uo, uf))):
        copies.append(pltpu.make_async_copy(source, target.at[pl.ds(n % 2 * 128, 128), :], sems.at[n + 1]))
    for copy in copies:
        copy.start()
    for copy in copies:
        copy.wait()
    st[:, :768] = product(vf[...], u[...], 1, 1).astype(LOW)
    st[:, 768:] = product(vf[...], uf[...], 1, 1).astype(LOW)
    side[...] = product(v[...], uf[...], 1, 1).astype(LOW)
    cols = columns_of(core)
    far = (product(st[:, :768], u[:, cols]) + product(st[:, 768:], uf[:, cols])).astype(LOW)
    up[...] = far[:, :1024]
    down[...] = far[:, 1024:]
    cubes = jnp.zeros((128, 128), WIDE)
    for n, by in enumerate((0, -1, 1, 2)):
        row = lax.rem(y + by * (1 - core) + SIDE, SIDE)
        column = lax.rem(x - by * core + SIDE, SIDE)
        block = pl.ds(pl.multiple_of(((row * SIDE + column) * 2 + core) * 128, 128), 128)
        left = near[n * 256 : n * 256 + 128, :] if n < 3 else st[:128, :768]
        right = side[n * 256 : n * 256 + 128, :] if n < 3 else st[:128, 768:]
        cubes += product(left, u[:, block]) + product(right, uf[:, block])
    eye = lax.broadcasted_iota(jnp.int32, (128, 128), 0) == lax.broadcasted_iota(jnp.int32, (128, 128), 1)
    trace[...] = jnp.full((8, 128), jnp.sum(jnp.where(eye, 1.5 * diagonal[...] - 0.5 * cubes, 0.0)))


def sums_body(u, near, side, uc, uo, up2, down2, own, up3, down3, uf, sems):
    cols = columns_of(lax.axis_index("core"))
    copies = [
        pltpu.make_async_copy(source.at[:, cols], uf.at[pl.ds(n * 128, 128), :], sems.at[n])
        for n, source in enumerate((uc, uo))
    ]
    for copy in copies:
        copy.start()
    for copy in copies:
        copy.wait()
    for n in (2, 1, 0):
        rows = slice(n * 256, n * 256 + 256)
        sums = product(near[rows, :], u[:, cols]) + product(side[rows, :], uf[...])
        if n == 2:
            up3[...] = sums[:, :1024]
            up2[...] = sums[:, 1024:].astype(LOW)
        elif n == 1:
            down2[...] = sums[:, :1024].astype(LOW)
            down3[...] = sums[:, 1024:]
        else:
            own[...] = sums


def early_body(here, there, exact, out):
    core = lax.axis_index("core")
    for part, place in ((here, core), (there, 1 - core)):
        cols = columns_of(place)
        out[:, cols] = 1.5 * exact[:, cols] - 0.5 * part[...]


def late_body(early, up, down, up_there, down_there, out):
    core = lax.axis_index("core")
    for first, last, place in ((up, down, core), (up_there, down_there, 1 - core)):
        for n, part in enumerate((first, last)):
            cols = pl.ds(pl.multiple_of(place * 2048 + n * 1024, 128), 1024)
            out[:, cols] = early[:, cols] - 0.5 * part[...].astype(WIDE)


def dma(n):
    return pltpu.SemaphoreType.DMA((n,))


def step(hamiltonian):
    rows, order = hamiltonian.shape
    half, quarter = order // 2, order // 4
    block = hamiltonian.astype(LOW)
    ua, va = move(block, "u", 1), move(block, "v", 1)
    other = swap(block)
    ub, vb = move(other, "u", 1), move(other, "v", 1)
    uf, vf = move(ua, "u", 1), move(va, "v", 1)
    sua, sva, sub, svb = swap(ua), swap(va), swap(ub), swap(vb)
    suf, svf = swap(uf), swap(vf)
    v_near = [block, other, va, vb, sub, sua]
    u_near = [block, other, ua, ub, svb, sva]

    v, u, near = kernel(
        near_body, v_near + u_near, [ANY] * 12,
        [((768, order), LOW), ((768, order), LOW), ((768, 768), LOW)], [dma(12)], 24, 4_800_000_000,
    )
    side, up, down, total = kernel(
        far_body, [v, u, near, vf, suf, uf, svf, hamiltonian], [VMEM] * 3 + [ANY] * 5,
        [((768, 256), LOW), ((256, quarter), LOW), ((256, quarter), LOW), ((8, 128), WIDE)],
        [pltpu.VMEM((256, order), LOW)] * 2 + [pltpu.VMEM((256, 1024), LOW), pltpu.VMEM((128, 128), WIDE), dma(5)],
        28, 5_000_000_000,
    )
    up2, down2, own, up3, down3 = kernel(
        sums_body, [u, near, side, uf, svf], [VMEM] * 3 + [ANY] * 2,
        [((256, quarter), LOW)] * 2 + [((256, half), WIDE)] + [((256, quarter), WIDE)] * 2,
        [pltpu.VMEM((256, half), LOW), dma(2)], 24, 3_300_000_000,
    )

    up, down = move(up, "v", 1), move(down, "v", -1)
    up2, down2 = move(up2, "v", 1), move(down2, "v", -1)
    up3 = move((up3 + up.astype(WIDE)).astype(LOW), "v", 1)
    down3 = move((down3 + down.astype(WIDE)).astype(LOW), "v", -1)
    sums = own + jnp.concatenate([down2, up2], axis=1).astype(WIDE)
    there = swap(sums[rows:])
    (early,) = kernel(
        early_body, [sums[:rows], there, hamiltonian], [VMEM] * 3, [((rows, order), WIDE)], [], 12, 1_000_000_000
    )
    parts = [up3[:rows], down3[:rows], swap(up3[rows:]), swap(down3[rows:])]
    (sign_next,) = kernel(late_body, [early, *parts], [VMEM] * 5, [((rows, order), WIDE)], [], 12, 1_000_000_000)
    for axis, by in (("core", 1), ("x", 1), ("x", 2), ("y", 1), ("y", 2)):
        total = total + shift(total, axis, by)
    return sign_next, 0.5 - total[0, :1] / (2.0 * order)


def solution(mesh):
    grid = Mesh(mesh.devices.reshape(mesh.shape["ka"], SIDE, SIDE, 2), ("ka", *GRID))
    rows = P(("ka", *GRID), None)
    return jax.shard_map(step, mesh=grid, in_specs=(rows,), out_specs=(rows, P("ka")), check_vma=False)
```

```python
import jax
import jax.numpy as jnp
from jax import lax
from jax.experimental import pallas as pl
from jax.experimental.pallas import tpu as pltpu
from jax.sharding import Mesh
from jax.sharding import PartitionSpec as P

LOW = jnp.bfloat16
WIDE = jnp.float32
ANY = pl.BlockSpec(memory_space=pl.ANY)
HBM = pl.BlockSpec(memory_space=pltpu.HBM)
VMEM = pl.BlockSpec(memory_space=pltpu.VMEM)
SIDE = 4
SPLIT = 1024
GRID = ("y", "x", "core")


def moved(y, x, core, axis, by):
    by = by if core == 0 else -by
    if (axis == "u") == (core == 0):
        return y, (x + by) % SIDE, core
    return (y + by) % SIDE, x, core


def index(y, x, core):
    return (y * SIDE + x) * 2 + core


PLACES = [(y, x, core) for y in range(SIDE) for x in range(SIDE) for core in range(2)]


def move(array, axis, by):
    return lax.ppermute(array, GRID, [(index(*p), index(*moved(*p, axis, by))) for p in PLACES])


def shift(array, axis, by):
    size = lax.axis_size(axis)
    return lax.ppermute(array, axis, [(i, (i + by) % size) for i in range(size)])


def swap(array):
    return shift(array, "core", 1)


def product(a, b, left=1, right=0):
    return lax.dot_general(a, b, (((left,), (right,)), ((), ())), preferred_element_type=WIDE)


def kernel(body, args, specs, outs, scratch, limit, flops, out_specs=None):
    return pl.pallas_call(
        body,
        out_shape=[jax.ShapeDtypeStruct(*out) for out in outs],
        in_specs=specs,
        out_specs=out_specs or [VMEM] * len(outs),
        scratch_shapes=scratch,
        compiler_params=pltpu.CompilerParams(vmem_limit_bytes=limit << 20),
        cost_estimate=pl.CostEstimate(flops=flops, bytes_accessed=1 << 20, transcendentals=0),
    )(*args)


def gather(sources, targets, sems):
    copies = [pltpu.make_async_copy(a, b, sems.at[n]) for n, (a, b) in enumerate(zip(sources, targets))]
    for copy in copies:
        copy.start()
    for copy in copies:
        copy.wait()


def join_body(one, two, out, sems):
    gather([one, two], [out.at[pl.ds(0, 128), :], out.at[pl.ds(128, 128), :]], sems)


def by_blocks(count, body):
    @pl.loop(0, count)
    def _(n):
        body(pl.ds(pl.multiple_of(n * 256, 256), 256))


def halves_of(target, row):
    return [target.at[pl.ds(row, 128), pl.ds(n * 2048, 2048)] for n in (0, 1)]


def gather_blocks(pieces, v, u, sems, halves):
    count = len(pieces) // len(halves)
    sources, targets = [], []
    for n in range(len(halves)):
        b, o, *rest = pieces[n * count : (n + 1) * count]
        for target, shift in ((v, 0), (u, 1)):
            column = [b, o]
            for k in range(0, len(rest), 3):
                column += [rest[k + shift], rest[k + 2].at[pl.ds(128 * shift, 128), :]]
            sources += column
            targets += [target.at[pl.ds(k * 128, 128), pl.ds(n * 2048, 2048)] for k in range(len(column))]
    gather(sources, targets, sems)


def first_body(*refs):
    pieces, (out, v, u, sems) = refs[:10], refs[10:]
    gather_blocks(pieces, v, u, sems, (0, 1))

    def block(rows):
        out[rows, :] = product(v[rows, :], u[...], 1, 1).astype(LOW)

    by_blocks(2, block)


def low_body(*refs):
    pieces, (rows, side, v, u, sems) = refs[:8], refs[8:]
    gather_blocks(pieces, v, u, sems, (0,))
    rows[...] = product(v[512:, :], u[...], 1, 1)

    def block(part):
        side[part, :] = product(v[part, :], u[512:, :], 1, 1)

    by_blocks(2, block)


def near_body(*refs):
    pieces, (done, rows, side, v, u, out, sems) = refs[:16], refs[16:]
    gather_blocks(pieces, v, u, sems, (0, 1))
    out[:512, :512] = done[...]
    out[512:, :] = (product(v[512:, 2048:], u[:, 2048:], 1, 1) + rows[...]).astype(LOW)
    out[:512, 512:] = (product(v[:512, 2048:], u[512:, 2048:], 1, 1) + side[...]).astype(LOW)


def half_body(v, u, vc, uc, far, rows, side, vf, uf, sems):
    sources = (vc, far.at[pl.ds(0, 128), :], uc, far.at[pl.ds(128, 128), :])
    gather(sources, [f.at[pl.ds(n, 128), :] for f in (vf, uf) for n in (0, 128)], sems)
    rows[:, :768] = product(vf[...], u[:, :2048], 1, 1)
    rows[:, 768:] = product(vf[...], uf[...], 1, 1)
    side[...] = product(v[:, :2048], uf[...], 1, 1)


def columns_of(core):
    return pl.ds(pl.multiple_of(core * 2048, 128), 2048)


BLOCKS = ((0, 1), (2, 4), (5, 3))


def far_body(*refs):
    v, u, near, rows_half, side_half, vc, uc, far, uc_low, far_low, exact = refs[:11]
    side, up, down, trace, uf, vf, st, diagonal, sems = refs[11:]
    y, x, core = (lax.axis_index(a) for a in GRID)
    own = pl.multiple_of(((y * SIDE + x) * 2 + core) * 128, 128)
    low, high = pl.ds(0, 128), pl.ds(128, 128)
    sources = [exact.at[:, pl.ds(own, 128)], vc, far.at[low, :], uc_low, uc, far_low.at[high, :], far.at[high, :]]
    gather(sources, [diagonal, vf.at[low, :], vf.at[high, :], *halves_of(uf, 0), *halves_of(uf, 128)], sems)
    st[:, :768] = (product(vf[...], u[:, 2048:], 1, 1) + rows_half[:, :768]).astype(LOW)
    st[:, 768:] = (product(vf[...], uf[:, 2048:], 1, 1) + rows_half[:, 768:]).astype(LOW)
    side[...] = (product(v[:, 2048:], uf[:, 2048:], 1, 1) + side_half[...]).astype(LOW)
    cols = columns_of(core)
    far = (product(st[:, :768], u[:, cols]) + product(st[:, 768:], uf[:, cols])).astype(LOW)
    up[:256, :] = far[:, :SPLIT]
    down[:256, :] = far[:, SPLIT:]
    cubes = jnp.zeros((128, 128), WIDE)
    for n, by in enumerate((0, -1, 1, 2)):
        row = lax.rem(y + by * (1 - core) + SIDE, SIDE)
        column = lax.rem(x - by * core + SIDE, SIDE)
        block = pl.ds(pl.multiple_of(((row * SIDE + column) * 2 + core) * 128, 128), 128)
        start = BLOCKS[n][0] * 128 if n < 3 else 0
        left = near[start : start + 128, :] if n < 3 else st[:128, :768]
        right = side[start : start + 128, :] if n < 3 else st[:128, 768:]
        cubes += product(left, u[:, block]) + product(right, uf[:, block])
    eye = lax.broadcasted_iota(jnp.int32, (128, 128), 0) == lax.broadcasted_iota(jnp.int32, (128, 128), 1)
    total = jnp.full((16, 128), jnp.sum(jnp.where(eye, 1.5 * diagonal[...] - 0.5 * cubes, 0.0)))
    trace[...] = total[:8]
    for n in range(3):
        term = total.astype(LOW)
        total = total - term.astype(WIDE)
        for message in (up, down):
            message[256:, n * 128 : (n + 1) * 128] = term
    for message in (up, down):
        message[256:, 384:] = jnp.zeros((16, message.shape[1] - 384), LOW)


def block_sums(n, u, near, side, uf):
    cols = columns_of(lax.axis_index("core"))
    left = jnp.concatenate([near[k * 128 : k * 128 + 128, :] for k in BLOCKS[n]], axis=0)
    right = jnp.concatenate([side[k * 128 : k * 128 + 128, :] for k in BLOCKS[n]], axis=0)
    return product(left, u[:, cols]) + product(right, uf[:, cols])


def sides_body(u, near, side, uf, ahead, ahead_later, behind, behind_later):
    sums = block_sums(2, u, near, side, uf)
    ahead_later[...] = sums[:, :SPLIT]
    ahead[...] = sums[:, SPLIT:].astype(LOW)
    sums = block_sums(1, u, near, side, uf)
    behind[...] = sums[:, :SPLIT].astype(LOW)
    behind_later[...] = sums[:, SPLIT:]


def own_body(u, near, side, uf, own):
    own[...] = block_sums(0, u, near, side, uf)


def add_body(later, got, out, total):
    out[...] = (later[...] + got[:256, :].astype(WIDE)).astype(LOW)
    terms = got[256:, :384].astype(WIDE)
    total[...] = terms[:8, :128] + terms[:8, 128:256] + terms[:8, 256:]


def settle_body(own, down2, up2, here, there):
    for out, rows in ((here, slice(0, 128)), (there, slice(128, 256))):
        out[:, :SPLIT] = own[rows, :SPLIT] + down2[rows, :].astype(WIDE)
        out[:, SPLIT:] = own[rows, SPLIT:] + up2[rows, :].astype(WIDE)


def early_body(here, there, exact, out):
    core = lax.axis_index("core")
    for part, place in ((here, core), (there, 1 - core)):
        cols = columns_of(place)
        out[:, cols] = 1.5 * exact[:, cols] - 0.5 * part[...]


def late_body(early, up, down, late, total, swapped, out, occupation):
    core = lax.axis_index("core")
    first = pl.ds(pl.multiple_of(core * 2048, 128), SPLIT)
    last = pl.ds(pl.multiple_of(core * 2048 + SPLIT, 128), 2048 - SPLIT)
    for cols, part in ((first, up[:128, :]), (last, down[:128, :]), (columns_of(1 - core), late[...])):
        out[:, cols] = early[:, cols] - 0.5 * part.astype(WIDE)
    occupation[0] = 0.5 - jnp.max(total[...] + swapped[...]) / (2.0 * early.shape[1])


def dma(n):
    return pltpu.SemaphoreType.DMA((n,))


def step(hamiltonian):
    rows, order = hamiltonian.shape
    half = order // 2
    b = [hamiltonian[:, :half].astype(LOW), hamiltonian[:, half:].astype(LOW)]
    ua, va, o, ub, vb, uf, vf, sa, sb, sf = ([None, None] for _ in range(10))
    for n in (0, 1):
        ua[n], va[n] = move(b[n], "u", 1), move(b[n], "v", 1)
        o[n] = swap(b[n])
        ub[n], vb[n] = move(o[n], "u", 1), move(o[n], "v", 1)
        uf[n], vf[n] = move(ua[n], "u", 1), move(va[n], "v", 1)
        sa[n], sb[n], sf[n] = (
            swap(kernel(join_body, pair, [ANY] * 2, [((256, half), LOW)], [dma(2)], 2, 1_000_000)[0])
            for pair in ((ua[n], va[n]), (ub[n], vb[n]), (uf[n], vf[n]))
        )
    first = [[b[n], o[n], va[n], ua[n], sa[n]] for n in (0, 1)]
    both = [first[n] + [vb[n], ub[n], sb[n]] for n in (0, 1)]

    (near,) = kernel(
        first_body, first[0] + first[1], [ANY] * 10, [((512, 512), LOW)],
        [pltpu.VMEM((512, order), LOW)] * 2 + [dma(16)], 10, 2_100_000_000,
    )
    rows_low, side_low = kernel(
        low_body, both[0], [ANY] * 8,
        [((256, 768), WIDE), ((512, 256), WIDE)], [pltpu.VMEM((768, half), LOW)] * 2 + [dma(12)], 14, 1_300_000_000,
    )
    v, u, near = kernel(
        near_body, both[0] + both[1] + [near, rows_low, side_low], [ANY] * 16 + [VMEM] * 3,
        [((768, order), LOW), ((768, order), LOW), ((768, 768), LOW)], [dma(24)], 16, 1_300_000_000,
    )
    rows_half, side_half = kernel(
        half_body, [v, u, vf[0], uf[0], sf[0]], [VMEM] * 2 + [ANY] * 3,
        [((256, 1024), WIDE), ((768, 256), WIDE)], [pltpu.VMEM((256, half), LOW)] * 2 + [dma(4)], 8, 1_900_000_000,
    )
    side, up, down, total, far = kernel(
        far_body, [v, u, near, rows_half, side_half, vf[1], uf[1], sf[1], uf[0], sf[0], hamiltonian],
        [VMEM] * 5 + [ANY] * 5 + [HBM],
        [((768, 256), LOW), ((272, SPLIT), LOW), ((272, half - SPLIT), LOW), ((8, 128), WIDE), ((256, order), LOW)],
        [pltpu.VMEM((256, half), LOW), pltpu.VMEM((256, 1024), LOW)]
        + [pltpu.VMEM((128, 128), WIDE), dma(7)], 14, 3_300_000_000,
    )
    operands, small = [u, near, side, far], ((8, 128), WIDE)
    first, last = [((256, SPLIT), kind) for kind in (LOW, WIDE)], [((256, half - SPLIT), kind) for kind in (LOW, WIDE)]
    ahead, ahead_later, behind, behind_later = kernel(
        sides_body, operands, [VMEM] * 4, [last[0], first[1], first[0], last[1]], [], 12, 2_100_000_000
    )
    (own,) = kernel(own_body, operands, [VMEM] * 4, [((256, half), WIDE)], [], 8, 1_100_000_000)
    up, down = move(up, "v", 1), move(down, "v", -1)
    up2, down2 = move(ahead, "v", 1), move(behind, "v", -1)
    up3, up_total = kernel(add_body, [ahead_later, up], [VMEM] * 2, [first[0], small], [], 8, 1_000_000)
    down3, down_total = kernel(add_body, [behind_later, down], [VMEM] * 2, [last[0], small], [], 8, 1_000_000)
    total = total + up_total + down_total + move(total, "v", 2)
    up3, down3 = move(up3, "v", 1), move(down3, "v", -1)
    part = ((rows, half), WIDE)
    here, there = kernel(settle_body, [own, down2, up2], [VMEM] * 3, [part, part], [], 10, 1_000_000)
    (early,) = kernel(
        early_body, [here, swap(there), hamiltonian], [VMEM] * 3, [((rows, order), WIDE)], [], 8, 1_000_000
    )
    late = swap(jnp.concatenate([up3[rows:], down3[rows:]], axis=1))
    total = total + move(total, "u", 2)
    total = total + move(total, "u", 1)
    return kernel(
        late_body, [early, up3, down3, late, total, swap(total)], [VMEM] * 6,
        [((rows, order), WIDE), ((1,), WIDE)], [], 8, 2_000_000_000, [VMEM, pl.BlockSpec(memory_space=pltpu.SMEM)],
    )


def solution(mesh):
    grid = Mesh(mesh.devices.reshape(mesh.shape["ka"], SIDE, SIDE, 2), ("ka", *GRID))
    rows = P(("ka", *GRID), None)
    return jax.shard_map(step, mesh=grid, in_specs=(rows,), out_specs=(rows, P("ka")), check_vma=False)
```

```python
import jax
import jax.numpy as jnp
from jax import lax
from jax.experimental import pallas as pl
from jax.experimental.pallas import tpu as pltpu
from jax.sharding import Mesh
from jax.sharding import PartitionSpec as P

LOW = jnp.bfloat16
WIDE = jnp.float32
ANY = pl.BlockSpec(memory_space=pl.ANY)
HBM = pl.BlockSpec(memory_space=pltpu.HBM)
VMEM = pl.BlockSpec(memory_space=pltpu.VMEM)
SIDE = 4
SPLIT = 1024
GRID = ("y", "x", "core")


def moved(y, x, core, axis, by):
    by = by if core == 0 else -by
    if (axis == "u") == (core == 0):
        return y, (x + by) % SIDE, core
    return (y + by) % SIDE, x, core


def index(y, x, core):
    return (y * SIDE + x) * 2 + core


PLACES = [(y, x, core) for y in range(SIDE) for x in range(SIDE) for core in range(2)]


def move(array, axis, by):
    return lax.ppermute(array, GRID, [(index(*p), index(*moved(*p, axis, by))) for p in PLACES])


def shift(array, axis, by):
    size = lax.axis_size(axis)
    return lax.ppermute(array, axis, [(i, (i + by) % size) for i in range(size)])


def swap(array):
    return shift(array, "core", 1)


def product(a, b, left=1, right=0):
    return lax.dot_general(a, b, (((left,), (right,)), ((), ())), preferred_element_type=WIDE)


def kernel(body, args, specs, outs, scratch, limit, flops, out_specs=None, aliases=None):
    return pl.pallas_call(
        body,
        out_shape=[jax.ShapeDtypeStruct(*out) for out in outs],
        in_specs=specs,
        out_specs=out_specs or [VMEM] * len(outs),
        input_output_aliases=aliases or {},
        scratch_shapes=scratch,
        compiler_params=pltpu.CompilerParams(vmem_limit_bytes=limit << 20),
        cost_estimate=pl.CostEstimate(flops=flops, bytes_accessed=1 << 20, transcendentals=0),
    )(*args)


def gather(sources, targets, sems):
    copies = [pltpu.make_async_copy(a, b, sems.at[n]) for n, (a, b) in enumerate(zip(sources, targets))]
    for copy in copies:
        copy.start()
    for copy in copies:
        copy.wait()


def join_body(one, two, out, sems):
    gather([one, two], [out.at[pl.ds(0, 128), :], out.at[pl.ds(128, 128), :]], sems)


def by_blocks(count, body):
    @pl.loop(0, count)
    def _(n):
        body(pl.ds(pl.multiple_of(n * 256, 256), 256))


def halves_of(target, row):
    return [target.at[pl.ds(row, 128), pl.ds(n * 2048, 2048)] for n in (0, 1)]


def gather_blocks(pieces, v, u, sems, halves):
    count = len(pieces) // len(halves)
    sources, targets = [], []
    for n in range(len(halves)):
        b, o, *rest = pieces[n * count : (n + 1) * count]
        for target, shift in ((v, 0), (u, 1)):
            column = [b, o]
            for k in range(0, len(rest), 3):
                column += [rest[k + shift], rest[k + 2].at[pl.ds(128 * shift, 128), :]]
            sources += column
            targets += [target.at[pl.ds(k * 128, 128), pl.ds(n * 2048, 2048)] for k in range(len(column))]
    gather(sources, targets, sems)


def first_body(*refs):
    pieces, (out, v, u, sems) = refs[:10], refs[10:]
    gather_blocks(pieces, v, u, sems, (0, 1))

    def block(rows):
        out[rows, :] = product(v[rows, :], u[...], 1, 1).astype(LOW)

    by_blocks(2, block)


def low_body(*refs):
    pieces, (rows, side, v, u, sems) = refs[:8], refs[8:]
    gather_blocks(pieces, v, u, sems, (0,))
    rows[...] = product(v[512:, :], u[...], 1, 1)

    def block(part):
        side[part, :] = product(v[part, :], u[512:, :], 1, 1)

    by_blocks(2, block)


def near_body(*refs):
    pieces, (done, rows, side, v, u, out, sems) = refs[:16], refs[16:]
    gather_blocks(pieces, v, u, sems, (0, 1))
    out[:512, :512] = done[...]
    out[512:, :] = (product(v[512:, 2048:], u[:, 2048:], 1, 1) + rows[...]).astype(LOW)
    out[:512, 512:] = (product(v[:512, 2048:], u[512:, 2048:], 1, 1) + side[...]).astype(LOW)


def half_body(v, u, vc, uc, far, rows, side, vf, uf, sems):
    sources = (vc, far.at[pl.ds(0, 128), :], uc, far.at[pl.ds(128, 128), :])
    gather(sources, [f.at[pl.ds(n, 128), :] for f in (vf, uf) for n in (0, 128)], sems)
    rows[:, :768] = product(vf[...], u[:, :2048], 1, 1)
    rows[:, 768:] = product(vf[...], uf[...], 1, 1)
    side[...] = product(v[:, :2048], uf[...], 1, 1)


def columns_of(core):
    return pl.ds(pl.multiple_of(core * 2048, 128), 2048)


BLOCKS = ((0, 1), (2, 4), (5, 3))


def columns_at(n):
    y, x, core = (lax.axis_index(a) for a in GRID)
    by = (0, -1, 1, 2)[n]
    row, column = lax.rem(y + by * (1 - core) + SIDE, SIDE), lax.rem(x - by * core + SIDE, SIDE)
    return pl.ds(pl.multiple_of(((row * SIDE + column) * 2 + core) * 128, 128), 128)


def sums_near_body(u, near, ahead, behind, cubes):
    cols = columns_of(lax.axis_index("core"))
    for out, blocks in ((ahead, BLOCKS[2]), (behind, BLOCKS[1])):
        left = jnp.concatenate([near[k * 128 : k * 128 + 128, :] for k in blocks], axis=0)
        out[...] = product(left, u[:, cols])
    total = jnp.zeros((128, 128), WIDE)
    for n in range(3):
        start = BLOCKS[n][0] * 128
        total += product(near[start : start + 128, :], u[:, columns_at(n)])
    cubes[...] = total


def far_body(*refs):
    v, u, cubes_near, rows_half, side_half, vc, uc, far, uc_low, far_low, exact = refs[:11]
    side, up, down, trace, uf, vf, st, diagonal, sems = refs[11:]
    y, x, core = (lax.axis_index(a) for a in GRID)
    own = pl.multiple_of(((y * SIDE + x) * 2 + core) * 128, 128)
    low, high = pl.ds(0, 128), pl.ds(128, 128)
    sources = [exact.at[:, pl.ds(own, 128)], vc, far.at[low, :], uc_low, uc, far_low.at[high, :], far.at[high, :]]
    gather(sources, [diagonal, vf.at[low, :], vf.at[high, :], *halves_of(uf, 0), *halves_of(uf, 128)], sems)
    st[:, :768] = (product(vf[...], u[:, 2048:], 1, 1) + rows_half[:, :768]).astype(LOW)
    st[:, 768:] = (product(vf[...], uf[:, 2048:], 1, 1) + rows_half[:, 768:]).astype(LOW)
    side[...] = (product(v[:, 2048:], uf[:, 2048:], 1, 1) + side_half[...]).astype(LOW)
    cols = columns_of(core)
    far = (product(st[:, :768], u[:, cols]) + product(st[:, 768:], uf[:, cols])).astype(LOW)
    up[:256, :] = far[:, :SPLIT]
    down[:256, :] = far[:, SPLIT:]
    cubes = cubes_near[...]
    for n in range(4):
        block = columns_at(n)
        start = BLOCKS[n][0] * 128 if n < 3 else 0
        if n == 3:
            cubes += product(st[:128, :768], u[:, block])
        cubes += product(side[start : start + 128, :] if n < 3 else st[:128, 768:], uf[:, block])
    eye = lax.broadcasted_iota(jnp.int32, (128, 128), 0) == lax.broadcasted_iota(jnp.int32, (128, 128), 1)
    total = jnp.full((16, 128), jnp.sum(jnp.where(eye, 1.5 * diagonal[...] - 0.5 * cubes, 0.0)))
    trace[...] = total[:8]
    for n in range(3):
        term = total.astype(LOW)
        total = total - term.astype(WIDE)
        for message in (up, down):
            message[256:, n * 128 : (n + 1) * 128] = term
    for message in (up, down):
        message[256:, 384:] = jnp.zeros((16, message.shape[1] - 384), LOW)


def block_sums(n, u, near, side, uf):
    cols = columns_of(lax.axis_index("core"))
    left = jnp.concatenate([near[k * 128 : k * 128 + 128, :] for k in BLOCKS[n]], axis=0)
    right = jnp.concatenate([side[k * 128 : k * 128 + 128, :] for k in BLOCKS[n]], axis=0)
    return product(left, u[:, cols]) + product(right, uf[:, cols])


def sides_body(ahead_near, behind_near, side, uf, ahead, ahead_later, behind, behind_later):
    cols = columns_of(lax.axis_index("core"))
    left = jnp.concatenate([side[k * 128 : k * 128 + 128, :] for k in BLOCKS[2] + BLOCKS[1]], axis=0)
    sums = product(left, uf[:, cols])
    ahead_later[...] = sums[:256, :SPLIT] + ahead_near[:, :SPLIT]
    ahead[...] = (sums[:256, SPLIT:] + ahead_near[:, SPLIT:]).astype(LOW)
    behind[...] = (sums[256:, :SPLIT] + behind_near[:, :SPLIT]).astype(LOW)
    behind_later[...] = sums[256:, SPLIT:] + behind_near[:, SPLIT:]


def own_body(u, near, side, uf, own):
    own[...] = block_sums(0, u, near, side, uf)


def add_body(later, got, out, total):
    out[...] = (later[...] + got[:256, :].astype(WIDE)).astype(LOW)
    terms = got[256:, :384].astype(WIDE)
    total[...] = terms[:8, :128] + terms[:8, 128:256] + terms[:8, 256:]


def settle_body(own, down2, up2, here, there):
    for out, rows in ((here, slice(0, 128)), (there, slice(128, 256))):
        out[:, :SPLIT] = own[rows, :SPLIT] + down2[rows, :].astype(WIDE)
        out[:, SPLIT:] = own[rows, SPLIT:] + up2[rows, :].astype(WIDE)


def early_body(here, there, exact, out):
    core = lax.axis_index("core")
    for part, place in ((here, core), (there, 1 - core)):
        cols = columns_of(place)
        out[:, cols] = 1.5 * exact[:, cols] - 0.5 * part[...]


def pair_body(up, down, out, sems):
    gather([up.at[pl.ds(128, 128), :], down.at[pl.ds(128, 128), :]], [out.at[:, pl.ds(0, SPLIT)], out.at[:, pl.ds(SPLIT, 2048 - SPLIT)]], sems)


CHUNK = 512


def finish(place, early, part, out, ready, sems):
    copies = []
    for n in range(2048 // CHUNK):
        here = pl.ds(n * CHUNK, CHUNK)
        cols = pl.ds(pl.multiple_of(place * 2048 + n * CHUNK, 128), CHUNK)
        ready[:, here] = early[:, cols] - 0.5 * part(n * CHUNK).astype(WIDE)
        copies.append(pltpu.make_async_copy(ready.at[:, here], out.at[:, cols], sems.at[n]))
        copies[-1].start()
    return copies


def here_body(early, up, down, out, ready, sems):
    def part(n):
        return up[:128, n : n + CHUNK] if n < SPLIT else down[:128, n - SPLIT : n - SPLIT + CHUNK]

    for copy in finish(lax.axis_index("core"), early, part, out, ready, sems):
        copy.wait()


def there_body(written, early, late, out, ready, sems):
    for copy in finish(1 - lax.axis_index("core"), early, lambda n: late[:, n : n + CHUNK], out, ready, sems):
        copy.wait()


def occupation_body(total, swapped, occupation):
    occupation[0] = 0.5 - jnp.max(total[...] + swapped[...]) / (2.0 * 4096)


def dma(n):
    return pltpu.SemaphoreType.DMA((n,))


def step(hamiltonian):
    rows, order = hamiltonian.shape
    half = order // 2
    low = hamiltonian[:, :half].astype(LOW)
    high = lax.optimization_barrier((hamiltonian, low))[0][:, half:].astype(LOW)
    b = [low, high]
    ua, va, o, ub, vb, uf, vf, sa, sb, sf = ([None, None] for _ in range(10))
    for n in (0, 1):
        ua[n], va[n] = move(b[n], "u", 1), move(b[n], "v", 1)
        o[n] = swap(b[n])
        ub[n], vb[n] = move(o[n], "u", 1), move(o[n], "v", 1)
        uf[n], vf[n] = move(ua[n], "u", 1), move(va[n], "v", 1)
        sa[n], sb[n], sf[n] = (
            swap(kernel(join_body, pair, [ANY] * 2, [((256, half), LOW)], [dma(2)], 2, 1_000_000)[0])
            for pair in ((ua[n], va[n]), (ub[n], vb[n]), (uf[n], vf[n]))
        )
    first = [[b[n], o[n], va[n], ua[n], sa[n]] for n in (0, 1)]
    both = [first[n] + [vb[n], ub[n], sb[n]] for n in (0, 1)]

    (near,) = kernel(
        first_body, first[0] + first[1], [ANY] * 10, [((512, 512), LOW)],
        [pltpu.VMEM((512, order), LOW)] * 2 + [dma(16)], 10, 2_100_000_000,
    )
    rows_low, side_low = kernel(
        low_body, both[0], [ANY] * 8,
        [((256, 768), WIDE), ((512, 256), WIDE)], [pltpu.VMEM((768, half), LOW)] * 2 + [dma(12)], 14, 1_300_000_000,
    )
    v, u, near = kernel(
        near_body, both[0] + both[1] + [near, rows_low, side_low], [ANY] * 16 + [VMEM] * 3,
        [((768, order), LOW), ((768, order), LOW), ((768, 768), LOW)], [dma(24)], 16, 1_300_000_000,
    )
    rows_half, side_half = kernel(
        half_body, [v, u, vf[0], uf[0], sf[0]], [VMEM] * 2 + [ANY] * 3,
        [((256, 1024), WIDE), ((768, 256), WIDE)], [pltpu.VMEM((256, half), LOW)] * 2 + [dma(4)], 8, 1_900_000_000,
    )
    ahead_near, behind_near, cubes_near = kernel(
        sums_near_body, [u, near], [VMEM] * 2, [((256, half), WIDE)] * 2 + [((rows, rows), WIDE)], [], 8,
        1_700_000_000,
    )
    side, up, down, total, far = kernel(
        far_body, [v, u, cubes_near, rows_half, side_half, vf[1], uf[1], sf[1], uf[0], sf[0], hamiltonian],
        [VMEM] * 5 + [ANY] * 5 + [HBM],
        [((768, 256), LOW), ((272, SPLIT), LOW), ((272, half - SPLIT), LOW), ((8, 128), WIDE), ((256, order), LOW)],
        [pltpu.VMEM((256, half), LOW), pltpu.VMEM((256, 1024), LOW)]
        + [pltpu.VMEM((128, 128), WIDE), dma(7)], 14, 3_300_000_000,
    )
    operands, small = [u, near, side, far], ((8, 128), WIDE)
    first, last = [((256, SPLIT), kind) for kind in (LOW, WIDE)], [((256, half - SPLIT), kind) for kind in (LOW, WIDE)]
    ahead, ahead_later, behind, behind_later = kernel(
        sides_body, [ahead_near, behind_near, side, far], [VMEM] * 4, [last[0], first[1], first[0], last[1]], [], 12, 2_100_000_000
    )
    (own,) = kernel(own_body, operands, [VMEM] * 4, [((256, half), WIDE)], [], 8, 1_100_000_000)
    up, down = move(up, "v", 1), move(down, "v", -1)
    up2, down2 = move(ahead, "v", 1), move(behind, "v", -1)
    up3, up_total = kernel(add_body, [ahead_later, up], [VMEM] * 2, [first[0], small], [], 8, 1_000_000)
    down3, down_total = kernel(add_body, [behind_later, down], [VMEM] * 2, [last[0], small], [], 8, 1_000_000)
    total = total + up_total + down_total + move(total, "v", 2)
    up3, down3 = move(up3, "v", 1), move(down3, "v", -1)
    part = ((rows, half), WIDE)
    here, there = kernel(settle_body, [own, down2, up2], [VMEM] * 3, [part, part], [], 10, 1_000_000)
    (early,) = kernel(
        early_body, [here, swap(there), hamiltonian], [VMEM] * 3, [((rows, order), WIDE)], [], 8, 1_000_000
    )
    (pair,) = kernel(pair_body, [up3, down3], [ANY] * 2, [((rows, half), LOW)], [dma(2)], 2, 1_000_000)
    late = swap(pair)
    ready = [pltpu.VMEM((rows, half), WIDE), dma(half // CHUNK)]
    (sign_next,) = kernel(
        here_body, [early, up3, down3], [VMEM] * 3, [((rows, order), WIDE)], ready, 4, 1_000_000_000, [ANY]
    )
    total = total + move(total, "u", 1) + move(total, "u", -1) + move(total, "u", 2)
    (occupation,) = kernel(
        occupation_body, [total, swap(total)], [VMEM] * 2, [((1,), WIDE)], [], 2, 1_000_000,
        [pl.BlockSpec(memory_space=pltpu.SMEM)],
    )
    (sign_next,) = kernel(
        there_body, [sign_next, early, late], [ANY] + [VMEM] * 2, [((rows, order), WIDE)], ready, 4,
        1_000_000_000, [ANY], {0: 0},
    )
    return sign_next, occupation


def solution(mesh):
    grid = Mesh(mesh.devices.reshape(mesh.shape["ka"], SIDE, SIDE, 2), ("ka", *GRID))
    rows = P(("ka", *GRID), None)
    return jax.shard_map(step, mesh=grid, in_specs=(rows,), out_specs=(rows, P("ka")), check_vma=False)
```
